32 devices in a mesh: row: 4 (over z), col: 8 (over y, x, core).
Axes of the slice: x: 2, y: 2, z: 4, core: 2. Of those that a mesh axis runs over, the one named last changes fastest.
Arguments:
- eigen_basis_rows: float32 [8192, 4096], P('row', 'col'), may hold values from -6 to 6
- mirror_entries: float32 [6, 4, 128, 2176], P(None, 'row', 'col'), may hold values from -0.125 to 0.125
- tau_coefficients: float32 [6, 4, 128], P(None, 'row', 'col'), may hold values from 0.5 to 2
- mirror_tallies: int32 [6, 4], P(None, 'row'), may hold values from 32 to 128
Outputs:
- transformed: float32 [8192, 4096], P('row', 'col')
The draws below stay inside these ranges and needn't reach their ends.
All inputs are finite; a program needn't handle non-finite values.
Results may differ from the reference program's by a relative error of at most 0.00017.
Values sent between devices are 32-bit elements; how exact they have to be, the bound alone decides.
No kernel may reach another device: no remote copies, remote signals or barrier semaphores. Data moves between devices by JAX's collectives and lax.ppermute only.
A program may use at most 64 MiB of HBM per device.

```python
import math
import jax
import jax.numpy as jnp
from jax import lax

PANEL_EXTENT = 128
R_DEV = 2048
MIRROR_BATCHES = 6
WIN = 2176
ROWS = 8192
COLS = 4096
N_ROW = 4


def set_ends(array, key, smallest, high):
    extent = array.shape
    index_at = [jax.random.randint(jax.random.fold_in(key, axis), (), 0, extent[axis]) for axis in range(len(extent))]
    array = array.at[tuple(index_at)].set(smallest)
    longest = extent.index(max(extent))
    index_at[longest] = (index_at[longest] + 1) % extent[longest]
    return array.at[tuple(index_at)].set(high)


def levels(own_key, extent, pieces, low, top_value):
    def one(position, blocks):
        heights = jax.random.uniform(jax.random.fold_in(jax.random.fold_in(own_key, 6), position), (blocks,), jnp.float32, low / len(pieces), top_value / len(pieces))
        return jnp.repeat(jnp.exp(heights), extent[position] // blocks).reshape((-1,) + (1,) * (len(extent) - position - 1))

    factor_of = one(*pieces[0])
    for cut in pieces[1:]:
        factor_of = factor_of * one(*cut)
    return factor_of


def centred(own_key, shape, width, reach, split=(), kind=jnp.bfloat16):
    drawn = width * jax.random.normal(own_key, shape, jnp.float32)
    if split:
        drawn = drawn * levels(own_key, shape, split, -0.22, 0.18)
    return jnp.clip(drawn, -reach, reach).astype(kind)


def setup_inputs(seed: int = 0) -> dict:
    seeds = jax.random.split(jax.random.key(seed), 5)
    return {
        "eigen_basis_rows": centred(seeds[0], (ROWS, COLS), 1.0, 6.0, ((0, 4), (1, 8)), jnp.float32),
        "mirror_entries": centred(seeds[1], (MIRROR_BATCHES, N_ROW, PANEL_EXTENT, WIN), WIN ** -0.5, 0.125, ((1, 4), (2, 8)), jnp.float32),
        "tau_coefficients": jnp.clip(jnp.exp(math.log(2.0) - 1.3862944 * jax.random.uniform(seeds[2], (MIRROR_BATCHES, N_ROW, PANEL_EXTENT), jnp.float32) ** levels(seeds[2], (MIRROR_BATCHES, N_ROW, PANEL_EXTENT), ((1, 4), (2, 8)), -0.2, 0.2)), 0.5, 2.0),
        "mirror_tallies": set_ends(jax.random.randint(seeds[3], (MIRROR_BATCHES, N_ROW), PANEL_EXTENT // 4, PANEL_EXTENT + 1), jax.random.fold_in(seeds[3], 1), PANEL_EXTENT // 4, PANEL_EXTENT).astype(jnp.int32),
    }


PRECISE = lax.Precision.HIGHEST


def storage_triangle(mirror_directions, scaling, retention_flags):
    gram_matrix = lax.dot_general(mirror_directions, mirror_directions, (((1,), (1,)), ((), ())), precision=PRECISE, preferred_element_type=jnp.float32)
    diag_inverse = jnp.where(retention_flags, scaling, jnp.ones_like(scaling))
    nilpotent = diag_inverse[:, None] * jnp.triu(gram_matrix, 1)
    order_count = mirror_directions.shape[0]
    identity = jnp.eye(order_count, dtype=jnp.float32)
    power_term = -nilpotent
    inverse_part = identity + power_term
    reached = 1
    while 2 * reached < order_count:
        power_term = jnp.dot(power_term, power_term, precision=PRECISE, preferred_element_type=jnp.float32)
        inverse_part = inverse_part + jnp.dot(inverse_part, power_term, precision=PRECISE, preferred_element_type=jnp.float32)
        reached = reached * 2
    return inverse_part * diag_inverse[None, :]


def apply_block(window, mirror_directions, triangle_operator):
    coeffs = jnp.dot(mirror_directions, window, precision=PRECISE, preferred_element_type=jnp.float32)
    mixed_terms = jnp.dot(triangle_operator, coeffs, precision=PRECISE, preferred_element_type=jnp.float32)
    return window - lax.dot_general(mirror_directions, mixed_terms, (((0,), (0,)), ((), ())), precision=PRECISE, preferred_element_type=jnp.float32)


def reference(eigen_basis_rows, mirror_entries, tau_coefficients, mirror_tallies):
    column_count = eigen_basis_rows.shape[1]
    padded = jnp.concatenate([eigen_basis_rows, jnp.zeros((PANEL_EXTENT, column_count), jnp.float32)], axis=0)
    slot_index = jnp.arange(PANEL_EXTENT, dtype=jnp.int32)
    cell_index = jnp.arange(WIN, dtype=jnp.int32)
    for batch_ordinal in range(MIRROR_BATCHES):
        for panel_ordinal in range(N_ROW):
            retention_flags = slot_index < mirror_tallies[batch_ordinal, panel_ordinal]
            if panel_ordinal == N_ROW - 1:
                row_keep = cell_index < R_DEV
            else:
                row_keep = cell_index >= 0
            mirror_directions = mirror_entries[batch_ordinal, panel_ordinal] * retention_flags[:, None].astype(jnp.float32) * row_keep[None, :].astype(jnp.float32)
            triangle_operator = storage_triangle(mirror_directions, tau_coefficients[batch_ordinal, panel_ordinal], retention_flags)
            first_row = panel_ordinal * R_DEV
            window = apply_block(padded[first_row:first_row + WIN], mirror_directions, triangle_operator)
            padded = padded.at[first_row:first_row + WIN].set(window)
    return padded[:N_ROW * R_DEV]
```

```python
import jax
import jax.numpy as jnp
from jax import lax
from jax.sharding import PartitionSpec as P

FINE = lax.Precision.HIGHEST
GOOD = lax.Precision.HIGH


def mm(a, b, dims=((1,), (0,)), precision=GOOD):
    return lax.dot_general(
        a, b, (dims, ((), ())), precision=precision, preferred_element_type=jnp.float32
    )


def gather_shards(x):
    size = lax.axis_size("col")
    me = lax.axis_index("col")
    if size & (size - 1) or size < 2:
        return lax.all_gather(x, "col", axis=0), jnp.arange(size, dtype=jnp.int32)
    flips = list(range(0, size, 2))
    mine = [x] + [
        lax.ppermute(x, "col", [(j, j ^ flip) for j in range(size)]) for flip in flips[1:]
    ]
    near = jnp.stack(mine)
    far = lax.ppermute(near, "col", [(j, j ^ 1) for j in range(size)])
    order = jnp.array(flips + [flip ^ 1 for flip in flips], jnp.int32)
    return jnp.concatenate([near, far]), me.astype(jnp.int32) ^ order


def factor(gram, dinv, before):
    count = gram.shape[0]
    power = -dinv[:, None] * jnp.where(before, gram, 0.0)
    inverse = jnp.eye(count, dtype=jnp.float32) + power
    reached = 1
    while 2 * reached < count:
        power = mm(power, power, precision=FINE)
        inverse = inverse + mm(inverse, power, precision=FINE)
        reached *= 2
    return inverse * dinv[None, :]


def neighbour_swaps(even, odd, position):
    count = lax.axis_size("row")

    def swap(block, first):
        pairs = [(i, i + 1) for i in range(first, count - 1, 2)]
        if not pairs:
            return jnp.zeros_like(block)
        return lax.ppermute(block, "row", pairs + [(b, a) for a, b in pairs])

    return swap(even, 0), swap(odd, 1)


def per_device(rows, entries, tau, tallies):
    sections = lax.axis_size("row")
    position = lax.axis_index("row").astype(jnp.int32)
    groups, _, width, window = entries.shape
    depth, columns = rows.shape
    shared = window - depth
    half = columns // 2
    odd = position % 2

    tag = jnp.broadcast_to(tau[:, 0, :, None], (groups, width, 128))
    stacked, owners = gather_shards(jnp.concatenate([entries[:, 0], tag], axis=2))
    count = width * stacked.shape[0]
    ids = (owners[:, None] * width + jnp.arange(width, dtype=jnp.int32)[None, :]).reshape(count)
    stacked = jnp.swapaxes(stacked, 0, 1).reshape(groups, count, window + 128)
    scales = stacked[:, :, window]
    live = ids[None, :] < tallies
    cells = jnp.arange(window, dtype=jnp.int32)
    kept = (cells < depth) | (position != sections - 1)
    vectors = jnp.where(live[:, :, None] & kept[None, None, :], stacked[:, :, :window], 0.0)
    inner = vectors[:, :, shared:depth].reshape(groups * count, depth - shared)
    edges = jnp.concatenate([vectors[:, :, :shared], vectors[:, :, depth:]], axis=2)

    before = ids[:, None] < ids[None, :]
    gram = mm(inner, inner, ((1,), (1,))).reshape(groups, count, groups * count)
    factors = []
    for g in range(groups):
        whole = gram[g, :, g * count : (g + 1) * count] + mm(edges[g], edges[g], ((1,), (1,)))
        factors.append(factor(whole, jnp.where(live[g], scales[g], 1.0), before))
    factors = jnp.stack(factors)

    lower = rows[shared:]
    product = mm(inner, lower).reshape(groups, count, columns)

    def part(block, label):
        start = half * ((label + position) % 2)
        return lax.dynamic_slice_in_dim(block, start, half, axis=block.ndim - 1)

    tops = [part(rows[:shared], label) for label in (0, 1)]
    products = [part(product, label) for label in (0, 1)]
    mixed = [jnp.zeros((groups + 1, count, half), jnp.float32) for _ in (0, 1)]

    def cross(above, below):
        even = jnp.where(odd == 0, below, above)
        uneven = jnp.where(odd == 0, above, below)
        even, uneven = neighbour_swaps(even, uneven, position)
        return jnp.where(odd == 0, uneven, even), jnp.where(odd == 0, even, uneven)

    steps = 2 * (groups - 1) + sections + 1
    from_above, from_below = cross(tops[1], tops[1])
    from_above = tops[0]
    for step in range(steps):
        label = step % 2
        g = jnp.floor_divide(step - position, 2)
        active = (g >= 0) & (g < groups)
        slot = jnp.where(active, g, groups)
        g = jnp.clip(g, 0, groups - 1)
        top = jnp.where(position == 0, tops[label], from_above) if step else from_above
        pair = jnp.concatenate([top, from_below], axis=0)
        sofar = mixed[label][:groups].reshape(groups * count, half)
        edge = lax.dynamic_index_in_dim(edges, g, 0, keepdims=False)
        base = lax.dynamic_index_in_dim(products[label], g, 0, keepdims=False)
        base = base - mm(lax.dynamic_index_in_dim(gram, g, 0, keepdims=False), sofar)
        coefficients = base + mm(edge, pair)
        answer = mm(lax.dynamic_index_in_dim(factors, g, 0, keepdims=False), coefficients)
        answer = jnp.where(active, answer, 0.0)
        pair = pair - mm(edge, answer, ((0,), (0,)))
        mixed[label] = lax.dynamic_update_index_in_dim(mixed[label], answer, slot, 0)
        tops[label] = jnp.where(active, pair[:shared], tops[label])
        if step < steps - 1:
            from_above, from_below = cross(pair[:shared], pair[shared:])

    def whole_width(pieces):
        left = jnp.where(odd == 0, pieces[0], pieces[1])
        right = jnp.where(odd == 0, pieces[1], pieces[0])
        return jnp.concatenate([left, right], axis=1)

    answers = whole_width([m[:groups].reshape(groups * count, half) for m in mixed])
    lower = lower - mm(inner, answers, ((0,), (0,)))
    return jnp.concatenate([whole_width(tops), lower], axis=0)


def solution(mesh):
    in_specs = (P("row", "col"), P(None, "row", "col", None), P(None, "row", "col"), P(None, "row"))
    return jax.shard_map(
        per_device, mesh=mesh, in_specs=in_specs, out_specs=P("row", "col"), check_vma=False
    )
```

```python
import functools

import jax
import jax.numpy as jnp
from jax import lax
from jax.experimental import pallas as pl
from jax.experimental.pallas import tpu as pltpu
from jax.sharding import PartitionSpec as P


FINE = lax.Precision.HIGHEST
GOOD = lax.Precision.HIGH
LANES = 128
ROW_BLOCK = 512
VMEM_BYTES = 20 * 1024 * 1024


def mm(a, b, dims=((1,), (0,)), precision=GOOD):
    return lax.dot_general(
        a, b, (dims, ((), ())), precision=precision, preferred_element_type=jnp.float32
    )


def halves(x):
    lead = x.astype(jnp.bfloat16)
    return lead, (x - lead.astype(jnp.float32)).astype(jnp.bfloat16)


def mm3(a, b, dims=((1,), (0,))):
    def one(p, q):
        return lax.dot_general(p, q, (dims, ((), ())), preferred_element_type=jnp.float32)

    return one(a[0], b[0]) + (one(a[0], b[1]) + one(a[1], b[0]))


def tie(x, *others):
    return lax.optimization_barrier((x, *others))[0]


def send_chips(x):
    size = lax.axis_size("col")
    return [x] + [
        lax.ppermute(x, "col", [(j, j ^ flip) for j in range(size)]) for flip in range(2, size, 2)
    ]


def send_cores(near):
    size = lax.axis_size("col")
    return near + [lax.ppermute(x, "col", [(j, j ^ 1) for j in range(size)]) for x in near]


def shard_order():
    size = lax.axis_size("col")
    me = lax.axis_index("col").astype(jnp.int32)
    flips = list(range(0, size, 2))
    return me ^ jnp.array(flips + [flip ^ 1 for flip in flips], jnp.int32)


def split_kernel(x_ref, lead_ref, trail_ref):
    lead_ref[...], trail_ref[...] = halves(x_ref[...])


def split(x):
    depth, columns = x.shape
    spec = pl.BlockSpec((ROW_BLOCK, columns), lambda i: (i, 0))
    shape = jax.ShapeDtypeStruct(x.shape, jnp.bfloat16)
    return pl.pallas_call(
        split_kernel,
        grid=(depth // ROW_BLOCK,),
        in_specs=[spec],
        out_specs=[spec, spec],
        out_shape=[shape, shape],
        compiler_params=pltpu.CompilerParams(vmem_limit_bytes=VMEM_BYTES),
        cost_estimate=pl.CostEstimate(flops=x.size * 2000, bytes_accessed=x.size * 8, transcendentals=0),
        name="split",
    )(x)


def prepare_kernel(group, at, shared, depth, shard_count, *refs):
    shards, refs = refs[:shard_count], refs[shard_count:]
    earlier, refs = refs[: 2 * group], refs[2 * group :]
    row_lead, row_trail, before, live, kept, refs = *refs[:5], refs[5:]
    if group:
        scales_in, refs = refs[0], refs[1:]
    lead_out, trail_out, edge_out, factor_out, product_out, refs = *refs[:5], refs[5:]
    if group:
        gram_out, refs = refs[0], refs[1:]
    else:
        scales_out, refs = refs[0], refs[1:]
    fresh, sems = refs
    count, window = lead_out.shape
    width = count // shard_count

    arrivals = [
        pltpu.make_async_copy(
            s.at[pl.ds(at * width, width)], fresh.at[pl.ds(i * width, width)], sems.at[i]
        )
        for i, s in enumerate(shards)
    ]
    for copy in arrivals:
        copy.start()
    for copy in arrivals:
        copy.wait()

    if group:
        scales = scales_in[...]
    else:
        scales = fresh[:, window : window + LANES]
        scales_out[...] = scales
    alive = live[...]
    whole = jnp.where(alive[:, group : group + 1] > 0.0, fresh[:, :window], 0.0) * kept[...]
    edge_out[...] = jnp.concatenate([whole[:, :shared], whole[:, depth:]], axis=1)
    both = halves(whole)
    lead_out[...], trail_out[...] = both
    turned = both[0].T, both[1].T

    gram = mm3(both, turned)
    flags = jnp.where(alive > 0.0, scales, 1.0)
    down = flags[:, group : group + 1]
    across = flags.T[group : group + 1]
    same = lax.broadcasted_iota(jnp.int32, (count, count), 0) == lax.broadcasted_iota(
        jnp.int32, (count, count), 1
    )
    inner = both[0][:, shared:depth], both[1][:, shared:depth]
    turned = turned[0][shared:depth], turned[1][shared:depth]
    power = -down * (gram * before[...])
    inverse = jnp.where(same, 1.0, 0.0) + power
    product_out[...] = mm3(inner, (row_lead[shared:], row_trail[shared:]))
    reached = 1
    while 2 * reached < count:
        power = mm(power, power, precision=FINE)
        inverse = inverse + mm(inverse, power, precision=FINE)
        reached *= 2
    factor_out[...] = inverse * across
    for i in range(group):
        past = [earlier[2 * i + j][:, shared:depth] for j in (0, 1)]
        gram_out[i * count : (i + 1) * count] = mm3(past, turned)


def prepare(group, shards, at, width, earlier, rows, shared, before, live, kept, scales):
    depth, columns = rows[0].shape
    window = kept.shape[1]
    count = width * len(shards)
    near = pl.BlockSpec(memory_space=pltpu.VMEM)
    inputs = [*shards, *[part for pair in earlier for part in pair], *rows, before, live, kept]
    if group:
        inputs.append(scales)
    f32 = lambda *shape: jax.ShapeDtypeStruct(shape, jnp.float32)
    half = jax.ShapeDtypeStruct((count, window), jnp.bfloat16)
    out_shape = [half, half, f32(count, 2 * shared), f32(count, count), f32(count, columns)]
    out_shape.append(f32(group * count, count) if group else f32(count, LANES))
    return pl.pallas_call(
        functools.partial(prepare_kernel, group, at, shared, depth, len(shards)),
        in_specs=[pl.BlockSpec(memory_space=pl.ANY)] * len(shards) + [near] * (len(inputs) - len(shards)),
        out_specs=[near] * 6,
        out_shape=out_shape,
        scratch_shapes=[
            pltpu.VMEM((count, shards[0].shape[1]), jnp.float32),
            pltpu.SemaphoreType.DMA((len(shards),)),
        ],
        compiler_params=pltpu.CompilerParams(vmem_limit_bytes=VMEM_BYTES),
        cost_estimate=pl.CostEstimate(
            flops=2_000_000_000, bytes_accessed=8_000_000, transcendentals=0
        ),
    )(*inputs)


def update_kernel(pieces, rows_ref, answers_ref, *refs):
    vectors, (out_ref, lead, trail) = refs[: 2 * pieces], refs[2 * pieces :]

    @pl.when(pl.program_id(0) == 0)
    def _():
        lead[...], trail[...] = halves(answers_ref[...])

    both = (
        jnp.concatenate([v[...] for v in vectors[::2]]),
        jnp.concatenate([v[...] for v in vectors[1::2]]),
    )
    out_ref[...] = rows_ref[...] - mm3(both, (lead[...], trail[...]), ((0,), (0,)))


def update(rows, answers, vectors):
    depth, columns = rows.shape
    count = vectors[0][0].shape[0]
    row_spec = pl.BlockSpec((ROW_BLOCK, columns), lambda i: (i, 0))
    return pl.pallas_call(
        functools.partial(update_kernel, len(vectors)),
        grid=(depth // ROW_BLOCK,),
        in_specs=[row_spec, pl.BlockSpec(answers.shape, lambda i: (0, 0))]
        + [pl.BlockSpec((count, ROW_BLOCK), lambda i: (0, i))] * (2 * len(vectors)),
        out_specs=row_spec,
        out_shape=jax.ShapeDtypeStruct(rows.shape, jnp.float32),
        scratch_shapes=[pltpu.VMEM(answers.shape, jnp.bfloat16)] * 2,
        compiler_params=pltpu.CompilerParams(vmem_limit_bytes=VMEM_BYTES),
        cost_estimate=pl.CostEstimate(
            flops=6 * answers.shape[0] * rows.size, bytes_accessed=rows.size * 8, transcendentals=0
        ),
        name="update",
    )(rows, answers, *[part for pair in vectors for part in pair])


def neighbour_swaps(even, odd):
    count = lax.axis_size("row")

    def swap(block, first):
        pairs = [(i, i + 1) for i in range(first, count - 1, 2)]
        if not pairs:
            return jnp.zeros_like(block)
        return lax.ppermute(block, "row", pairs + [(b, a) for a, b in pairs])

    return swap(even, 0), swap(odd, 1)


def cuts(groups):
    ends = [1, 1 + (groups - 1) // 2, groups]
    starts = [0] + ends[:-1]
    return [(a, b) for a, b in zip(starts, ends) if a < b]


def pick(choices, index):
    keys = sorted(choices)
    chosen = choices[keys[0]]
    for key in keys[1:]:
        chosen = jnp.where(index >= key, choices[key], chosen)
    return chosen


def transform(rows, entries, tau, tallies):
    sections = lax.axis_size("row")
    position = lax.axis_index("row").astype(jnp.int32)
    groups, _, width, window = entries.shape
    depth, columns = rows.shape
    shared = window - depth
    half = columns // 2
    odd = position % 2
    pieces = cuts(groups)
    piece_of = {g: (k, g - a) for k, (a, b) in enumerate(pieces) for g in range(a, b)}

    def part(block, label):
        start = half * ((label + position) % 2)
        return lax.dynamic_slice_in_dim(block, start, half, axis=block.ndim - 1)

    def cross(above, below):
        even = jnp.where(odd == 0, below, above)
        uneven = jnp.where(odd == 0, above, below)
        even, uneven = neighbour_swaps(even, uneven)
        return jnp.where(odd == 0, uneven, even), jnp.where(odd == 0, even, uneven)

    def block_of(k):
        first, last = pieces[k]
        return entries[first:last, 0].reshape((last - first) * width, window)

    cells = jnp.arange(window, dtype=jnp.int32)
    kept = ((cells < depth) | (position != sections - 1)).astype(jnp.float32)[None, :]
    owners = shard_order()
    count = width * owners.shape[0]
    ids = (owners[:, None] * width + jnp.arange(width, dtype=jnp.int32)[None, :]).reshape(count)
    live = (ids[:, None] < tallies.reshape(1, groups)).astype(jnp.float32)
    live = jnp.pad(live, ((0, 0), (0, LANES - groups)))
    before = (ids[:, None] < ids[None, :]).astype(jnp.float32)

    tag = jnp.pad(tau[:, 0, :].T, ((0, 0), (0, LANES - groups)))
    blocks = {k: block_of(k) for k in range(1, len(pieces))}
    near = {0: send_chips(jnp.concatenate([block_of(0), tag], axis=1))}
    split_rows = split(rows)
    tops = [part(rows[:shared], label) for label in (0, 1)]
    _, from_below = cross(tops[1], tops[1])
    held = lax.optimization_barrier((*near[0], from_below, *split_rows, *blocks.values()))
    near[0], from_below, split_rows = held[: len(near[0])], held[len(near[0])], held[-2 - len(blocks) :][:2]
    blocks = dict(zip(blocks, held[-len(blocks) :]))
    shards = {0: send_cores(list(near[0]))}
    if len(pieces) > 1:
        near[1] = send_chips(blocks[1])

    ready = {}
    scales = None

    def make(g, *after):
        k, at = piece_of[g]
        ours = lax.optimization_barrier((*shards[k], *after))[: len(shards[k])]
        earlier = [ready[h][:2] for h in range(g)]
        return prepare(g, ours, at, width, earlier, split_rows, shared, before, live, kept, scales)

    mixed = [jnp.zeros((groups + 1, count, half), jnp.float32) for _ in (0, 1)]
    from_above = tops[0]
    *ready[0], scales = make(0)

    slots = {max(1, 2 * g - 2): g for g in range(1, groups)}
    steps = 2 * (groups - 1) + sections + 1
    split_at = max(1, groups - 2)
    update_at = min(steps - 2, 2 * (split_at - 1) + sections + 1)
    full = rows

    def whole_width(first, last):
        pair = [m[first:last].reshape(-1, half) for m in mixed]
        left = jnp.where(odd == 0, pair[0], pair[1])
        right = jnp.where(odd == 0, pair[1], pair[0])
        return jnp.concatenate([left, right], axis=1)

    for step in range(steps):
        label = step % 2
        g = jnp.floor_divide(step - position, 2)
        active = (g >= 0) & (g < groups)
        slot = jnp.where(active, g, groups)
        near_by = sorted({min(max((step - r) // 2, 0), groups - 1) for r in range(sections)})
        choose = lambda f: pick({h: f(h) for h in near_by}, g)
        top = jnp.where(position == 0, tops[label], from_above) if step else from_above
        pair = jnp.concatenate([top, from_below], axis=0)
        edge = choose(lambda h: ready[h][2])
        base = part(choose(lambda h: ready[h][4]), label)
        known = near_by[-1]
        if known:
            strip = choose(
                lambda h: jnp.pad(ready[h][5], ((0, (known - h) * count), (0, 0)))
                if h
                else jnp.zeros((known * count, count), jnp.float32)
            )
            base = base - mm(strip, mixed[label][:known].reshape(known * count, half), ((0,), (0,)))
        coefficients = base + mm(edge, pair)
        answer = mm(choose(lambda h: ready[h][3]), coefficients)
        answer = lax.optimization_barrier(jnp.where(active, answer, 0.0))
        pair = pair - mm(edge, answer, ((0,), (0,)))
        mixed[label] = lax.dynamic_update_index_in_dim(mixed[label], answer, slot, 0)
        tops[label] = jnp.where(active, pair[:shared], tops[label])
        if step == steps - 1:
            break
        from_above, from_below = cross(pair[:shared], pair[shared:])
        for k in range(1, len(pieces)):
            if step == max(0, 2 * pieces[k][0] - 3):
                ours = lax.optimization_barrier((*near[k], pair))[:-1]
                shards[k] = send_cores(list(ours))
                if k + 1 < len(pieces):
                    near[k + 1] = send_chips(tie(blocks[k + 1], *ours))
        done = None
        if step in slots:
            fresh = slots[step]
            ready[fresh] = make(fresh, pair)
            done = ready[fresh]
        if step == update_at:
            done = [update(full, tie(whole_width(0, split_at), pair), [ready[h][:2] for h in range(split_at)])]
        if done is not None:
            held = lax.optimization_barrier((from_above, from_below, *done))
            from_above, from_below = held[:2]
            if step in slots:
                ready[fresh] = held[2:]
            else:
                full = held[2]

    full = update(full, whole_width(split_at, groups), [ready[h][:2] for h in range(split_at, groups)])
    left = jnp.where(odd == 0, tops[0], tops[1])
    right = jnp.where(odd == 0, tops[1], tops[0])
    return lax.dynamic_update_slice_in_dim(full, jnp.concatenate([left, right], axis=1), 0, 0)


def solution(mesh):
    in_specs = (P("row", "col"), P(None, "row", "col", None), P(None, "row", "col"), P(None, "row"))
    return jax.shard_map(transform, mesh=mesh, in_specs=in_specs, out_specs=P("row", "col"), check_vma=False)
```

```python
import functools

import jax
import jax.numpy as jnp
from jax import lax
from jax.experimental import pallas as pl
from jax.experimental.pallas import tpu as pltpu
from jax.sharding import PartitionSpec as P


FINE = lax.Precision.HIGHEST
GOOD = lax.Precision.HIGH
LANES = 128
ROW_BLOCK = 512
VMEM_BYTES = 20 * 1024 * 1024


def mm(a, b, dims=((1,), (0,)), precision=GOOD):
    return lax.dot_general(
        a, b, (dims, ((), ())), precision=precision, preferred_element_type=jnp.float32
    )


def halves(x):
    lead = x.astype(jnp.bfloat16)
    return lead, (x - lead.astype(jnp.float32)).astype(jnp.bfloat16)


def mm3(a, b, dims=((1,), (0,))):
    def one(p, q):
        return lax.dot_general(p, q, (dims, ((), ())), preferred_element_type=jnp.float32)

    return one(a[0], b[0]) + (one(a[0], b[1]) + one(a[1], b[0]))


def tie(x, *others):
    return lax.optimization_barrier((x, *others))[0]


def send_chips(x):
    size = lax.axis_size("col")
    return [x] + [
        lax.ppermute(x, "col", [(j, j ^ flip) for j in range(size)]) for flip in range(2, size, 2)
    ]


def send_cores(near):
    size = lax.axis_size("col")
    return near + [lax.ppermute(x, "col", [(j, j ^ 1) for j in range(size)]) for x in near]


def shard_order():
    size = lax.axis_size("col")
    me = lax.axis_index("col").astype(jnp.int32)
    flips = list(range(0, size, 2))
    return me ^ jnp.array(flips + [flip ^ 1 for flip in flips], jnp.int32)


def split_kernel(x_ref, lead_ref, trail_ref):
    lead_ref[...], trail_ref[...] = halves(x_ref[...])


def split(x):
    depth, columns = x.shape
    spec = pl.BlockSpec((ROW_BLOCK, columns), lambda i: (i, 0))
    shape = jax.ShapeDtypeStruct(x.shape, jnp.bfloat16)
    return pl.pallas_call(
        split_kernel,
        grid=(depth // ROW_BLOCK,),
        in_specs=[spec],
        out_specs=[spec, spec],
        out_shape=[shape, shape],
        compiler_params=pltpu.CompilerParams(vmem_limit_bytes=VMEM_BYTES),
        cost_estimate=pl.CostEstimate(flops=x.size * 2000, bytes_accessed=x.size * 8, transcendentals=0),
        name="split",
    )(x)


def prepare_kernel(group, at, shared, depth, shard_count, *refs):
    shards, refs = refs[:shard_count], refs[shard_count:]
    earlier, refs = refs[: 2 * group], refs[2 * group :]
    row_lead, row_trail, before, live, kept, refs = *refs[:5], refs[5:]
    if group:
        scales_in, refs = refs[0], refs[1:]
    lead_out, trail_out, edge_out, factor_out, product_out, refs = *refs[:5], refs[5:]
    if group:
        gram_out, refs = refs[0], refs[1:]
    else:
        scales_out, refs = refs[0], refs[1:]
    window, count = lead_out.shape
    width = count // shard_count
    mine = slice(at * width, (at + 1) * width)

    if group:
        scales = scales_in[...]
    else:
        scales = jnp.concatenate([s[mine, window : window + LANES] for s in shards])
        scales_out[...] = scales
    alive = live[...]
    whole = jnp.concatenate([s[mine, :window] for s in shards])
    whole = jnp.where(alive[:, group : group + 1] > 0.0, whole, 0.0) * kept[...]
    edge_out[...] = jnp.concatenate([whole[:, :shared], whole[:, depth:]], axis=1)
    both = halves(whole)
    turned = both[0].T, both[1].T
    lead_out[...], trail_out[...] = turned

    gram = mm3(both, turned)
    flags = jnp.where(alive > 0.0, scales, 1.0)
    down = flags[:, group : group + 1]
    across = flags.T[group : group + 1]
    same = lax.broadcasted_iota(jnp.int32, (count, count), 0) == lax.broadcasted_iota(
        jnp.int32, (count, count), 1
    )
    inner = both[0][:, shared:depth], both[1][:, shared:depth]
    power = -down * (gram * before[...])
    inverse = jnp.where(same, 1.0, 0.0) + power
    product_out[...] = mm3(inner, (row_lead[shared:], row_trail[shared:]))
    if count > 2:
        power = mm(power, power, precision=FINE)
    reached = 2
    while 2 * reached < count:
        level = mm(jnp.concatenate([power, inverse]), power, precision=FINE)
        power, inverse = level[:count], inverse + level[count:]
        reached *= 2
    if count > 2:
        inverse = inverse + mm(inverse, power, precision=FINE)
    factor_out[...] = inverse * across
    for i in range(0, group, 2):
        stop = min(i + 2, group)
        past = [
            jnp.concatenate([earlier[2 * h + j][shared:depth] for h in range(i, stop)], axis=1)
            for j in (0, 1)
        ]
        gram_out[:, i * count : stop * count] = mm3(inner, past)


def prepare(group, shards, at, width, earlier, rows, shared, before, live, kept, scales):
    depth, columns = rows[0].shape
    window = kept.shape[1]
    count = width * len(shards)
    near = pl.BlockSpec(memory_space=pltpu.VMEM)
    inputs = [*shards, *[part for pair in earlier for part in pair], *rows, before, live, kept]
    if group:
        inputs.append(scales)
    f32 = lambda *shape: jax.ShapeDtypeStruct(shape, jnp.float32)
    half = jax.ShapeDtypeStruct((window, count), jnp.bfloat16)
    out_shape = [half, half, f32(count, 2 * shared), f32(count, count), f32(count, columns)]
    out_shape.append(f32(count, group * count) if group else f32(count, LANES))
    return pl.pallas_call(
        functools.partial(prepare_kernel, group, at, shared, depth, len(shards)),
        in_specs=[near] * len(inputs),
        out_specs=[near] * 6,
        out_shape=out_shape,
        compiler_params=pltpu.CompilerParams(vmem_limit_bytes=VMEM_BYTES),
        cost_estimate=pl.CostEstimate(
            flops=2_000_000_000, bytes_accessed=8_000_000, transcendentals=0
        ),
    )(*inputs)


def update_kernel(pieces, rows_ref, answers_ref, *refs):
    vectors, (out_ref, lead, trail) = refs[: 2 * pieces], refs[2 * pieces :]

    @pl.when(pl.program_id(0) == 0)
    def _():
        lead[...], trail[...] = halves(answers_ref[...])

    both = (
        jnp.concatenate([v[...] for v in vectors[::2]], axis=1),
        jnp.concatenate([v[...] for v in vectors[1::2]], axis=1),
    )
    out_ref[...] = rows_ref[...] - mm3(both, (lead[...], trail[...]))


def update(rows, answers, vectors):
    depth, columns = rows.shape
    count = vectors[0][0].shape[1]
    row_spec = pl.BlockSpec((ROW_BLOCK, columns), lambda i: (i, 0))
    return pl.pallas_call(
        functools.partial(update_kernel, len(vectors)),
        grid=(depth // ROW_BLOCK,),
        in_specs=[row_spec, pl.BlockSpec(answers.shape, lambda i: (0, 0))]
        + [pl.BlockSpec((ROW_BLOCK, count), lambda i: (i, 0))] * (2 * len(vectors)),
        out_specs=row_spec,
        out_shape=jax.ShapeDtypeStruct(rows.shape, jnp.float32),
        scratch_shapes=[pltpu.VMEM(answers.shape, jnp.bfloat16)] * 2,
        compiler_params=pltpu.CompilerParams(vmem_limit_bytes=VMEM_BYTES),
        cost_estimate=pl.CostEstimate(
            flops=6 * answers.shape[0] * rows.size, bytes_accessed=rows.size * 8, transcendentals=0
        ),
        name="update",
    )(rows, answers, *[part for pair in vectors for part in pair])


def finish_kernel(pieces, place_ref, rows_ref, answers_ref, tops_ref, *refs):
    vectors, (out_ref, lead, trail) = refs[: 2 * pieces], refs[2 * pieces :]
    first = pl.program_id(0) == 0

    @pl.when(first)
    def _():
        lead[...], trail[...] = halves(answers_ref[...])

    both = (
        jnp.concatenate([v[...] for v in vectors[::2]], axis=1),
        jnp.concatenate([v[...] for v in vectors[1::2]], axis=1),
    )
    out_ref[...] = rows_ref[...] - mm3(both, (lead[...], trail[...]))

    @pl.when(first)
    def _():
        out_ref[: tops_ref.shape[0]] = tops_ref[...]


def finish(rows, answers, tops, vectors, place):
    depth = rows.shape[0]
    count = vectors[0][0].shape[1]
    half = answers.shape[1]
    row_spec = pl.BlockSpec((ROW_BLOCK, half), lambda i, p: (i, p[0]))
    return pl.pallas_call(
        functools.partial(finish_kernel, len(vectors)),
        grid_spec=pltpu.PrefetchScalarGridSpec(
            num_scalar_prefetch=1,
            grid=(depth // ROW_BLOCK,),
            in_specs=[
                row_spec,
                pl.BlockSpec(answers.shape, lambda i, p: (0, 0)),
                pl.BlockSpec(tops.shape, lambda i, p: (0, 0)),
            ]
            + [pl.BlockSpec((ROW_BLOCK, count), lambda i, p: (i, 0))] * (2 * len(vectors)),
            out_specs=row_spec,
            scratch_shapes=[pltpu.VMEM(answers.shape, jnp.bfloat16)] * 2,
        ),
        out_shape=jax.ShapeDtypeStruct(rows.shape, jnp.float32),
        input_output_aliases={1: 0},
        compiler_params=pltpu.CompilerParams(vmem_limit_bytes=VMEM_BYTES),
        cost_estimate=pl.CostEstimate(
            flops=6 * answers.size * depth, bytes_accessed=depth * half * 8, transcendentals=0
        ),
        name="finish",
    )(place, rows, answers, tops, *[part for pair in vectors for part in pair])


def neighbour_swaps(even, odd):
    count = lax.axis_size("row")

    def swap(block, first):
        pairs = [(i, i + 1) for i in range(first, count - 1, 2)]
        if not pairs:
            return jnp.zeros_like(block)
        return lax.ppermute(block, "row", pairs + [(b, a) for a, b in pairs])

    even = swap(even, 0)
    odd = swap(odd, 1)
    return even, odd


def cuts(groups):
    ends = [1, 2, 2 + (groups - 1) // 2, groups]
    starts = [0] + ends[:-1]
    return [(a, b) for a, b in zip(starts, ends) if a < b]


def windows(groups, sections):
    firsts = [a for a, _ in cuts(groups)]
    slots = {2 * g - (1 if g in firsts else 2): g for g in range(1, groups)}
    split_at = max(1, groups - 2)
    return 2 * (groups - 1) + sections + 1, slots, split_at, 2 * (split_at - 1) + sections


def pick(choices, index):
    keys = sorted(choices)
    chosen = choices[keys[0]]
    for key in keys[1:]:
        chosen = jnp.where(index >= key, choices[key], chosen)
    return chosen


def transform(rows, entries, tau, tallies):
    sections = lax.axis_size("row")
    position = lax.axis_index("row").astype(jnp.int32)
    groups, _, width, window = entries.shape
    depth, columns = rows.shape
    shared = window - depth
    half = columns // 2
    odd = position % 2
    pieces = cuts(groups)
    piece_of = {g: (k, g - a) for k, (a, b) in enumerate(pieces) for g in range(a, b)}

    def part(block, label):
        start = half * ((label + position) % 2)
        return lax.dynamic_slice_in_dim(block, start, half, axis=block.ndim - 1)

    def cross(above, below):
        even = jnp.where(odd == 0, below, above)
        uneven = jnp.where(odd == 0, above, below)
        even, uneven = neighbour_swaps(even, uneven)
        return jnp.where(odd == 0, uneven, even), jnp.where(odd == 0, even, uneven)

    def block_of(k):
        first, last = pieces[k]
        return entries[first:last, 0].reshape((last - first) * width, window)

    cells = jnp.arange(window, dtype=jnp.int32)
    kept = ((cells < depth) | (position != sections - 1)).astype(jnp.float32)[None, :]
    owners = shard_order()
    count = width * owners.shape[0]
    ids = (owners[:, None] * width + jnp.arange(width, dtype=jnp.int32)[None, :]).reshape(count)
    live = (ids[:, None] < tallies.reshape(1, groups)).astype(jnp.float32)
    live = jnp.pad(live, ((0, 0), (0, LANES - groups)))
    before = (ids[:, None] < ids[None, :]).astype(jnp.float32)

    tag = jnp.pad(tau[:, 0, :].T, ((0, 0), (0, LANES - groups)))
    blocks = {k: block_of(k) for k in range(1, len(pieces))}
    near = {0: send_chips(jnp.concatenate([block_of(0), tag], axis=1))}
    split_rows = split(rows)
    tops = [part(rows[:shared], label) for label in (0, 1)]
    _, from_below = cross(tops[1], tops[1])
    held = lax.optimization_barrier((*near[0], from_below, *blocks.values()))
    near[0], from_below = held[: len(near[0])], held[len(near[0])]
    blocks = dict(zip(blocks, held[-len(blocks) :]))
    shards = {0: send_cores(list(near[0]))}
    if len(pieces) > 1:
        near[1] = send_chips(blocks[1])

    ready = {}
    scales = None

    def make(g, *after):
        k, at = piece_of[g]
        ours = lax.optimization_barrier((*shards[k], *after))[: len(shards[k])]
        earlier = [ready[h][:2] for h in range(g)]
        return prepare(g, ours, at, width, earlier, split_rows, shared, before, live, kept, scales)

    mixed = [jnp.zeros((groups + 1, count, half), jnp.float32) for _ in (0, 1)]
    from_above = tops[0]
    *ready[0], scales = make(0)

    steps, slots, split_at, update_at = windows(groups, sections)
    full = rows

    def whole_width(first, last):
        pair = [m[first:last].reshape(-1, half) for m in mixed]
        left = jnp.where(odd == 0, pair[0], pair[1])
        right = jnp.where(odd == 0, pair[1], pair[0])
        return jnp.concatenate([left, right], axis=1)

    def end_half(full, label, *after):
        answers = tie(mixed[label][split_at:groups].reshape(-1, half), *after)
        place = ((label + position) % 2).reshape(1)
        return finish(full, answers, tops[label], [ready[h][:2] for h in range(split_at, groups)], place)

    for step in range(steps):
        label = step % 2
        g = jnp.floor_divide(step - position, 2)
        active = (g >= 0) & (g < groups)
        slot = jnp.where(active, g, groups)
        near_by = sorted({min(max((step - r) // 2, 0), groups - 1) for r in range(sections)})
        choose = lambda f: pick({h: f(h) for h in near_by}, g)
        top = jnp.where(position == 0, tops[label], from_above) if step else from_above
        pair = jnp.concatenate([top, from_below], axis=0)
        edge = choose(lambda h: ready[h][2])
        base = part(choose(lambda h: ready[h][4]), label)
        known = near_by[-1]
        if known:
            strip = choose(
                lambda h: jnp.pad(ready[h][5], ((0, 0), (0, (known - h) * count)))
                if h
                else jnp.zeros((count, known * count), jnp.float32)
            )
            base = base - mm(strip, mixed[label][:known].reshape(known * count, half))
        coefficients = base + mm(edge, pair)
        answer = mm(choose(lambda h: ready[h][3]), coefficients)
        answer = lax.optimization_barrier(jnp.where(active, answer, 0.0))
        pair = pair - mm(edge, answer, ((0,), (0,)))
        mixed[label] = lax.dynamic_update_index_in_dim(mixed[label], answer, slot, 0)
        tops[label] = jnp.where(active, pair[:shared], tops[label])
        if step == steps - 1:
            break
        from_above, from_below = cross(pair[:shared], pair[shared:])
        for k in range(1, len(pieces)):
            if step == 2 * pieces[k][0] - 2:
                ours = lax.optimization_barrier((*near[k], pair))[:-1]
                shards[k] = send_cores(list(ours))
                if k + 1 < len(pieces):
                    near[k + 1] = send_chips(tie(blocks[k + 1], *ours))
        done = None
        if step == steps - 2:
            done = [end_half(full, label, pair)]
        if step in slots:
            fresh = slots[step]
            ready[fresh] = make(fresh, pair)
            done = ready[fresh]
        if step == update_at:
            done = [update(full, tie(whole_width(0, split_at), pair), [ready[h][:2] for h in range(split_at)])]
        if done is not None:
            held = lax.optimization_barrier((from_above, from_below, *done))
            from_above, from_below = held[:2]
            if step in slots:
                ready[fresh] = held[2:]
            else:
                full = held[2]

    return end_half(full, label)


def solution(mesh):
    in_specs = (P("row", "col"), P(None, "row", "col", None), P(None, "row", "col"), P(None, "row"))
    return jax.shard_map(transform, mesh=mesh, in_specs=in_specs, out_specs=P("row", "col"), check_vma=False)
```

```python
import functools

import jax
import jax.numpy as jnp
from jax import lax
from jax.experimental import pallas as pl
from jax.experimental.pallas import tpu as pltpu
from jax.sharding import PartitionSpec as P


GOOD = lax.Precision.HIGH
LANES = 128
ROW_BLOCK = 512
VMEM_BYTES = 20 * 1024 * 1024


def mm(a, b, dims=((1,), (0,)), precision=GOOD):
    return lax.dot_general(
        a, b, (dims, ((), ())), precision=precision, preferred_element_type=jnp.float32
    )


def halves(x):
    lead = x.astype(jnp.bfloat16)
    return lead, (x - lead.astype(jnp.float32)).astype(jnp.bfloat16)


def mm3(a, b, dims=((1,), (0,))):
    def one(p, q):
        return lax.dot_general(p, q, (dims, ((), ())), preferred_element_type=jnp.float32)

    return one(a[0], b[0]) + (one(a[0], b[1]) + one(a[1], b[0]))


def tie(x, *others):
    return lax.optimization_barrier((x, *others))[0]


def send_chips(x):
    size = lax.axis_size("col")
    return [x] + [
        lax.ppermute(x, "col", [(j, j ^ flip) for j in range(size)]) for flip in range(2, size, 2)
    ]


def send_cores(near):
    size = lax.axis_size("col")
    return near + [lax.ppermute(x, "col", [(j, j ^ 1) for j in range(size)]) for x in near]


def shard_order():
    size = lax.axis_size("col")
    me = lax.axis_index("col").astype(jnp.int32)
    flips = list(range(0, size, 2))
    return me ^ jnp.array(flips + [flip ^ 1 for flip in flips], jnp.int32)


def split_kernel(x_ref, lead_ref, trail_ref):
    lead_ref[...], trail_ref[...] = halves(x_ref[...])


def split(x):
    depth, columns = x.shape
    spec = pl.BlockSpec((ROW_BLOCK, columns), lambda i: (i, 0))
    shape = jax.ShapeDtypeStruct(x.shape, jnp.bfloat16)
    return pl.pallas_call(
        split_kernel,
        grid=(depth // ROW_BLOCK,),
        in_specs=[spec],
        out_specs=[spec, spec],
        out_shape=[shape, shape],
        compiler_params=pltpu.CompilerParams(vmem_limit_bytes=VMEM_BYTES),
        cost_estimate=pl.CostEstimate(flops=x.size * 2000, bytes_accessed=x.size * 8, transcendentals=0),
        name="split",
    )(x)


def prepare_kernel(group, at, shared, depth, shard_count, *refs):
    shards, refs = refs[:shard_count], refs[shard_count:]
    earlier, refs = refs[: 2 * group], refs[2 * group :]
    row_lead, row_trail, before, live, kept, refs = *refs[:5], refs[5:]
    if group:
        scales_in, refs = refs[0], refs[1:]
    lead_out, trail_out, edge_out, factor_out, product_out, refs = *refs[:5], refs[5:]
    if group:
        gram_out, refs = refs[0], refs[1:]
    else:
        scales_out, refs = refs[0], refs[1:]
    window, count = lead_out.shape
    width = count // shard_count
    mine = slice(at * width, (at + 1) * width)

    if group:
        scales = scales_in[...]
    else:
        scales = jnp.concatenate([s[mine, window : window + LANES] for s in shards])
        scales_out[...] = scales
    alive = live[...]
    whole = jnp.concatenate([s[mine, :window] for s in shards])
    whole = jnp.where(alive[:, group : group + 1] > 0.0, whole, 0.0) * kept[...]
    edge_out[...] = jnp.concatenate([whole[:, :shared], whole[:, depth:]], axis=1)
    both = halves(whole)
    turned = both[0].T, both[1].T
    lead_out[...], trail_out[...] = turned

    gram = mm3(both, turned)
    flags = jnp.where(alive > 0.0, scales, 1.0)
    down = flags[:, group : group + 1]
    across = flags.T[group : group + 1]
    same = lax.broadcasted_iota(jnp.int32, (count, count), 0) == lax.broadcasted_iota(
        jnp.int32, (count, count), 1
    )
    inner = both[0][:, shared:depth], both[1][:, shared:depth]
    power = -down * (gram * before[...])
    inverse = jnp.where(same, 1.0, 0.0) + power

    def columns(n, _):
        at = pl.ds(pl.multiple_of(n * 2 * LANES, 2 * LANES), 2 * LANES)
        product_out[:, at] = mm3(inner, (row_lead[shared:, at], row_trail[shared:, at]))
        return 0

    lax.fori_loop(0, product_out.shape[1] // (2 * LANES), columns, 0)
    levels = max(0, (count - 1).bit_length() - 2)

    def level(state):
        power, inverse = state
        both = mm3(halves(jnp.concatenate([power, inverse])), halves(power))
        return both[:count], inverse + both[count:]

    power = mm3(halves(power), halves(power))
    for _ in range(levels):
        power, inverse = level((power, inverse))
    inverse = inverse + mm3(halves(inverse), halves(power))
    factor_out[...] = inverse * across
    for i in range(0, group, 2):
        stop = min(i + 2, group)
        past = [
            jnp.concatenate([earlier[2 * h + j][shared:depth] for h in range(i, stop)], axis=1)
            for j in (0, 1)
        ]
        gram_out[:, i * count : stop * count] = mm3(inner, past)


def prepare(group, shards, at, width, earlier, rows, shared, before, live, kept, scales):
    depth, columns = rows[0].shape
    window = kept.shape[1]
    count = width * len(shards)
    near = pl.BlockSpec(memory_space=pltpu.VMEM)
    inputs = [*shards, *[part for pair in earlier for part in pair], *rows, before, live, kept]
    if group:
        inputs.append(scales)
    f32 = lambda *shape: jax.ShapeDtypeStruct(shape, jnp.float32)
    half = jax.ShapeDtypeStruct((window, count), jnp.bfloat16)
    out_shape = [half, half, f32(count, 2 * shared), f32(count, count), f32(count, columns)]
    out_shape.append(f32(count, group * count) if group else f32(count, LANES))
    return pl.pallas_call(
        functools.partial(prepare_kernel, group, at, shared, depth, len(shards)),
        in_specs=[near] * len(inputs),
        out_specs=[near] * 6,
        out_shape=out_shape,
        compiler_params=pltpu.CompilerParams(vmem_limit_bytes=VMEM_BYTES),
        cost_estimate=pl.CostEstimate(
            flops=2_000_000_000, bytes_accessed=8_000_000, transcendentals=0
        ),
    )(*inputs)


def update_kernel(pieces, rows_ref, answers_ref, *refs):
    vectors, (out_ref, lead, trail) = refs[: 2 * pieces], refs[2 * pieces :]

    @pl.when(pl.program_id(0) == 0)
    def _():
        lead[...], trail[...] = halves(answers_ref[...])

    both = (
        jnp.concatenate([v[...] for v in vectors[::2]], axis=1),
        jnp.concatenate([v[...] for v in vectors[1::2]], axis=1),
    )
    out_ref[...] = rows_ref[...] - mm3(both, (lead[...], trail[...]))


def update(rows, answers, vectors):
    depth, columns = rows.shape
    count = vectors[0][0].shape[1]
    row_spec = pl.BlockSpec((ROW_BLOCK, columns), lambda i: (i, 0))
    return pl.pallas_call(
        functools.partial(update_kernel, len(vectors)),
        grid=(depth // ROW_BLOCK,),
        in_specs=[row_spec, pl.BlockSpec(answers.shape, lambda i: (0, 0))]
        + [pl.BlockSpec((ROW_BLOCK, count), lambda i: (i, 0))] * (2 * len(vectors)),
        out_specs=row_spec,
        out_shape=jax.ShapeDtypeStruct(rows.shape, jnp.float32),
        scratch_shapes=[pltpu.VMEM(answers.shape, jnp.bfloat16)] * 2,
        compiler_params=pltpu.CompilerParams(vmem_limit_bytes=VMEM_BYTES),
        cost_estimate=pl.CostEstimate(
            flops=6 * answers.shape[0] * rows.size, bytes_accessed=rows.size * 8, transcendentals=0
        ),
        name="update",
    )(rows, answers, *[part for pair in vectors for part in pair])


def finish_kernel(pieces, place_ref, rows_ref, answers_ref, tops_ref, *refs):
    vectors, (out_ref, buffer, sems) = refs[: 2 * pieces], refs[-3:]
    half = answers_ref.shape[1]
    at = pl.ds(pl.multiple_of(place_ref[0] * half, half), half)
    answers = halves(answers_ref[...])

    def out_copy(i):
        block = pl.ds(pl.multiple_of(i * ROW_BLOCK, ROW_BLOCK), ROW_BLOCK)
        return block, pltpu.make_async_copy(buffer.at[block], out_ref.at[block, at], sems.at[i])

    def make(i, _):
        block, copy = out_copy(i)
        both = [jnp.concatenate([v[block] for v in vectors[j::2]], axis=1) for j in (0, 1)]
        buffer[block] = rows_ref[block, at] - mm3(both, answers)

        @pl.when(i == 0)
        def _():
            buffer[: tops_ref.shape[0]] = tops_ref[...]

        copy.start()
        return 0

    def drain(i, _):
        out_copy(i)[1].wait()
        return 0

    blocks = rows_ref.shape[0] // ROW_BLOCK
    lax.fori_loop(0, blocks, make, 0)
    lax.fori_loop(0, blocks, drain, 0)


def finish(rows, answers, tops, vectors, place, out):
    near = pl.BlockSpec(memory_space=pltpu.VMEM)
    far = pl.BlockSpec(memory_space=pltpu.HBM)
    inputs = [place, rows, answers, tops, *[part for pair in vectors for part in pair]]
    in_specs = [pl.BlockSpec(memory_space=pltpu.SMEM)] + [near] * (len(inputs) - 1)
    if out is not None:
        inputs.append(out)
        in_specs.append(far)
    return pl.pallas_call(
        functools.partial(finish_kernel, len(vectors)),
        in_specs=in_specs,
        out_specs=far,
        out_shape=jax.ShapeDtypeStruct(rows.shape, jnp.float32),
        scratch_shapes=[
            pltpu.VMEM((rows.shape[0], answers.shape[1]), jnp.float32),
            pltpu.SemaphoreType.DMA((rows.shape[0] // ROW_BLOCK,)),
        ],
        input_output_aliases={} if out is None else {len(inputs) - 1: 0},
        compiler_params=pltpu.CompilerParams(vmem_limit_bytes=VMEM_BYTES),
        cost_estimate=pl.CostEstimate(
            flops=6 * answers.size * rows.shape[0], bytes_accessed=rows.size * 4, transcendentals=0
        ),
        name="finish",
    )(*inputs)


def neighbour_swaps(even, odd):
    count = lax.axis_size("row")

    def swap(block, first):
        pairs = [(i, i + 1) for i in range(first, count - 1, 2)]
        if not pairs:
            return jnp.zeros_like(block)
        return lax.ppermute(block, "row", pairs + [(b, a) for a, b in pairs])

    even = swap(even, 0)
    odd = swap(odd, 1)
    return even, odd


def cuts(groups):
    ends = [1, 2, groups]
    starts = [0] + ends[:-1]
    return [(a, b) for a, b in zip(starts, ends) if a < b]


def windows(groups, sections):
    firsts = [a for a, _ in cuts(groups)]
    slots = {2 * g - (1 if g in firsts else 2): g for g in range(1, groups)}
    split_at = max(1, groups - 2)
    return 2 * (groups - 1) + sections + 1, slots, split_at, 2 * (split_at - 1) + sections


def pick(choices, index):
    keys = sorted(choices)
    chosen = choices[keys[0]]
    for key in keys[1:]:
        chosen = jnp.where(index >= key, choices[key], chosen)
    return chosen


def transform(rows, entries, tau, tallies):
    sections = lax.axis_size("row")
    position = lax.axis_index("row").astype(jnp.int32)
    groups, _, width, window = entries.shape
    depth, columns = rows.shape
    shared = window - depth
    half = columns // 2
    odd = position % 2
    pieces = cuts(groups)
    piece_of = {g: (k, g - a) for k, (a, b) in enumerate(pieces) for g in range(a, b)}

    def part(block, label):
        start = half * ((label + position) % 2)
        return lax.dynamic_slice_in_dim(block, start, half, axis=block.ndim - 1)

    def cross(above, below):
        even = jnp.where(odd == 0, below, above)
        uneven = jnp.where(odd == 0, above, below)
        even, uneven = neighbour_swaps(even, uneven)
        return jnp.where(odd == 0, uneven, even), jnp.where(odd == 0, even, uneven)

    def block_of(k):
        first, last = pieces[k]
        return entries[first:last, 0].reshape((last - first) * width, window)

    cells = jnp.arange(window, dtype=jnp.int32)
    kept = ((cells < depth) | (position != sections - 1)).astype(jnp.float32)[None, :]
    owners = shard_order()
    count = width * owners.shape[0]
    ids = (owners[:, None] * width + jnp.arange(width, dtype=jnp.int32)[None, :]).reshape(count)
    live = (ids[:, None] < tallies.reshape(1, groups)).astype(jnp.float32)
    live = jnp.pad(live, ((0, 0), (0, LANES - groups)))
    before = (ids[:, None] < ids[None, :]).astype(jnp.float32)

    tag = jnp.pad(tau[:, 0, :].T, ((0, 0), (0, LANES - groups)))
    blocks = {k: block_of(k) for k in range(1, len(pieces))}
    near = {0: send_chips(jnp.concatenate([block_of(0), tag], axis=1))}
    if len(pieces) > 1:
        near[1] = send_chips(blocks.pop(1))
    split_rows = split(rows)
    tops = [part(rows[:shared], label) for label in (0, 1)]
    _, from_below = cross(tops[1], tops[1])
    held = lax.optimization_barrier((*near[0], from_below, *blocks.values()))
    near[0], from_below = held[: len(near[0])], held[len(near[0])]
    blocks = dict(zip(blocks, held[-len(blocks) :]))
    shards = {0: send_cores(list(near[0]))}
    for k, block in blocks.items():
        near[k] = send_chips(block)

    ready = {}
    scales = None

    def make(g, *after):
        k, at = piece_of[g]
        ours = lax.optimization_barrier((*shards[k], *after))[: len(shards[k])]
        earlier = [ready[h][:2] for h in range(g)]
        return prepare(g, ours, at, width, earlier, split_rows, shared, before, live, kept, scales)

    mixed = [jnp.zeros((groups + 1, count, half), jnp.float32) for _ in (0, 1)]
    from_above = tops[0]
    *ready[0], scales = make(0)

    steps, slots, split_at, update_at = windows(groups, sections)
    full = rows

    def whole_width(first, last):
        pair = [m[first:last].reshape(-1, half) for m in mixed]
        left = jnp.where(odd == 0, pair[0], pair[1])
        right = jnp.where(odd == 0, pair[1], pair[0])
        return jnp.concatenate([left, right], axis=1)

    def end_half(full, label, out, *after):
        answers = tie(mixed[label][split_at:groups].reshape(-1, half), *after)
        place = ((label + position) % 2).reshape(1)
        return finish(full, answers, tops[label], [ready[h][:2] for h in range(split_at, groups)], place, out)

    for step in range(steps):
        label = step % 2
        g = jnp.floor_divide(step - position, 2)
        active = (g >= 0) & (g < groups)
        slot = jnp.where(active, g, groups)
        near_by = sorted({min(max((step - r) // 2, 0), groups - 1) for r in range(sections)})
        choose = lambda f: pick({h: f(h) for h in near_by}, g)
        top = jnp.where(position == 0, tops[label], from_above) if step else from_above
        pair = jnp.concatenate([top, from_below], axis=0)
        edge = choose(lambda h: ready[h][2])
        base = part(choose(lambda h: ready[h][4]), label)
        known = near_by[-1]
        if known:
            strip = choose(
                lambda h: jnp.pad(ready[h][5], ((0, 0), (0, (known - h) * count)))
                if h
                else jnp.zeros((count, known * count), jnp.float32)
            )
            base = base - mm(strip, mixed[label][:known].reshape(known * count, half))
        coefficients = base + mm(edge, pair)
        answer = mm(choose(lambda h: ready[h][3]), coefficients)
        answer = lax.optimization_barrier(jnp.where(active, answer, 0.0))
        pair = pair - mm(edge, answer, ((0,), (0,)))
        mixed[label] = lax.dynamic_update_index_in_dim(mixed[label], answer, slot, 0)
        tops[label] = jnp.where(active, pair[:shared], tops[label])
        if step == steps - 1:
            break
        from_above, from_below = cross(pair[:shared], pair[shared:])
        for k in range(1, len(pieces)):
            if step == 2 * pieces[k][0] - 2:
                ours = lax.optimization_barrier((*near[k], pair))[:-1]
                shards[k] = send_cores(list(ours))
        done = None
        if step == steps - 2:
            done = [end_half(full, label, None, pair)]
        if step in slots:
            fresh = slots[step]
            ready[fresh] = make(fresh, pair)
            done = ready[fresh]
        if step == update_at:
            done = [update(full, tie(whole_width(0, split_at), pair), [ready[h][:2] for h in range(split_at)])]
        if done is not None:
            held = lax.optimization_barrier((from_above, from_below, *done))
            from_above, from_below = held[:2]
            if step in slots:
                ready[fresh] = held[2:]
            elif step == update_at:
                full = held[2]
            else:
                out = held[2]

    return end_half(full, label, out)


def solution(mesh):
    in_specs = (P("row", "col"), P(None, "row", "col", None), P(None, "row", "col"), P(None, "row"))
    return jax.shard_map(transform, mesh=mesh, in_specs=in_specs, out_specs=P("row", "col"), check_vma=False)
```
